256 devices in a mesh: blk: 128 (over y, z, x), grp: 2 (over core).
Axes of the slice: x: 4, y: 4, z: 8, core: 2. Of those that a mesh axis runs over, the one named last changes fastest.
Arguments:
- schur_blocks: bfloat16 [512, 1024, 1024], P(('blk', 'grp')), may hold values from -1 to 5, as said below
- residual: float32 [512, 1024, 128], P(('blk', 'grp')), may hold values from -200 to 200
- direction: float32 [512, 1024, 128], P(('blk', 'grp')), may hold values from -200 to 200
- corner_map: int32 [512, 24], P(('blk', 'grp')), may hold values from 0 to 63
- panel_order: int32 [8], replicated, may hold values from 0 to 7, each once
- coarse_factor: float32 [8, 8, 1024, 1024], P(None, None, 'blk'), may hold values from -0.0625 to 0.0625
- block_inverses: float32 [8, 1024, 1024], P(None, 'blk'), may hold values from -0.1875 to 0.1875
Outputs:
- residual_next: float32 [512, 1024, 128], P(('blk', 'grp'))
- direction_next: float32 [512, 1024, 128], P(('blk', 'grp'))
The draws below stay inside these ranges and needn't reach their ends.
Inputs may be any that keep to these rules, and one draw needn't show every extreme that they name: `schur_blocks`: each subdomain's block is symmetric positive definite. `panel_order`: each coarse block appears once.
All inputs are finite; a program needn't handle non-finite values.
Results may differ from the reference program's by a relative error of at most 0.0048.
Values sent between devices are 32-bit elements; how exact they have to be, the bound alone decides.
A program may use at most 64 MiB of HBM per device.

```python
import math
import jax
import jax.numpy as jnp
from jax import lax

NI = 1024
CB = 1024
PANELS = 8
COR = 24
NV = 128
SUB_DEV = 2
ITERS = 1
SUBS = 512
ROWS_B = 8
N_GRP = 2


def draw_schur_blocks(key, part):
    first_key, second_key = jax.random.split(jax.random.fold_in(key, 5))
    jitter = jax.random.normal(first_key, (SUBS, NI, NI))
    jitter = jnp.clip(jitter, -4.0, 4.0) * (0.18 / math.sqrt(NI))
    symmetric = jitter + jnp.swapaxes(jitter, 1, 2)
    diagonal = jnp.exp(jax.random.uniform(second_key, (SUBS, NI)) * math.log(4.0))
    identity = jnp.eye(NI, dtype=jnp.float32)
    return (symmetric + diagonal[:, :, None] * identity).astype(jnp.bfloat16)


def field_draw(key):
    first_key, second_key, third_key = jax.random.split(key, 3)
    growth = 3.0 ** (jnp.arange(SUBS, dtype=jnp.float32) / max(SUBS - 1, 1))
    row_scale = jnp.exp(jax.random.uniform(second_key, (SUBS, NI, 1)) * math.log(10.0))
    col_scale = jnp.exp(jax.random.uniform(third_key, (1, 1, NV)) * math.log(10.0))
    entries = jnp.clip(jax.random.normal(first_key, (SUBS, NI, NV)), -4.0, 4.0)
    return (entries * growth[:, None, None] * row_scale * col_scale / 20.0).astype(jnp.float32)


def draw_residual(key, part):
    return field_draw(jax.random.fold_in(key, 11))


def draw_direction(key, part):
    return field_draw(jax.random.fold_in(key, 23))


def set_ends(drawn, rng, least, top_value):
    index_at = [jax.random.randint(jax.random.fold_in(rng, axis), (), 0, length) for axis, length in enumerate(drawn.shape)]
    longest = drawn.shape.index(max(drawn.shape))
    neighbour = index_at[:longest] + [(index_at[longest] + 1) % drawn.shape[longest]] + index_at[longest + 1:]
    return drawn.at[tuple(index_at)].set(least).at[tuple(neighbour)].set(top_value)


def shard_levels(stream_key, dims, cuts, low, high):
    def one(axis_at, blocks):
        draws = jax.random.uniform(jax.random.fold_in(jax.random.fold_in(stream_key, 6), axis_at), (blocks,), jnp.float32, low / len(cuts), high / len(cuts))
        return jnp.repeat(jnp.exp(draws), dims[axis_at] // blocks).reshape((-1,) + (1,) * (len(dims) - axis_at - 1))

    gain = one(*cuts[0])
    for cut in cuts[1:]:
        gain = gain * one(*cut)
    return gain


def centred(key, shape, deviation, bound, cuts=(), held_as=jnp.bfloat16):
    level = shard_levels(key, shape, cuts, -0.22, 0.18) if cuts else 1.0
    values = jax.random.normal(key, shape, jnp.float32) * deviation * level
    return jnp.minimum(jnp.maximum(values, -bound), bound).astype(held_as)


def setup_inputs(seed: int = 0) -> dict:
    splits = jax.random.split(jax.random.key(seed), 8)
    schur_blocks = draw_schur_blocks(jax.random.fold_in(splits[7], 71), 0)
    residual = draw_residual(jax.random.fold_in(splits[7], 71), 0)
    direction = draw_direction(jax.random.fold_in(splits[7], 71), 0)
    corner_map = set_ends(jax.random.randint(splits[3], (SUBS, COR), 0, PANELS * ROWS_B), jax.random.fold_in(splits[3], 1), 0, (PANELS * ROWS_B) - 1).astype(jnp.int32)
    panel_order = jax.random.permutation(splits[4], PANELS).astype(jnp.int32)
    coarse_factor = centred(splits[5], (PANELS, PANELS, CB, CB), (PANELS * CB) ** -0.5, 0.0625, ((2, 128),), jnp.float32)
    block_inverses = centred(splits[6], (PANELS, CB, CB), CB ** -0.5, 0.1875, ((1, 128),), jnp.float32)
    return dict(schur_blocks=schur_blocks, residual=residual, direction=direction, corner_map=corner_map, panel_order=panel_order, coarse_factor=coarse_factor, block_inverses=block_inverses)


precise = lax.Precision.HIGHEST


def coarse_solve(coarse, panel_order, coarse_factor, block_inverses):
    solved = jnp.zeros_like(coarse)
    for position in range(PANELS):
        current = panel_order[position]
        target = coarse[current]
        for earlier in range(position):
            earlier_block = panel_order[earlier]
            target = target - jnp.dot(coarse_factor[current, earlier_block], solved[earlier_block], precision=precise)
        block_value = jnp.dot(block_inverses[current], target, precision=precise)
        solved = solved.at[current].set(block_value)
    return solved


def reference(schur_blocks, residual, direction, corner_map, panel_order, coarse_factor, block_inverses):
    sub_count = schur_blocks.shape[0]
    columns_count = residual.shape[2]
    owners = jnp.arange(sub_count, dtype=jnp.int32) // (SUB_DEV * N_GRP)
    coarse_index = (corner_map // ROWS_B) * CB + owners[:, None] * ROWS_B + corner_map % ROWS_B
    coarse_index = coarse_index.reshape(-1).astype(jnp.int32)

    def matvec(pieces):
        matrix, operand = pieces
        rounded = operand.astype(jnp.bfloat16).astype(jnp.float32)
        return jnp.dot(matrix.astype(jnp.float32), rounded, precision=precise)

    norm_now = jnp.sum(residual * residual, axis=(0, 1))
    for iteration in range(ITERS):
        applied = lax.map(matvec, (schur_blocks, direction))
        curvature = jnp.sum(direction * applied, axis=(0, 1))
        step_size = norm_now / curvature
        residual = residual - step_size * applied
        corner_vals = residual[:, :COR, :].reshape(-1, columns_count)
        coarse = jax.ops.segment_sum(corner_vals, coarse_index, num_segments=PANELS * CB)
        coarse = coarse.reshape(PANELS, CB, columns_count)
        solved = coarse_solve(coarse, panel_order, coarse_factor, block_inverses)
        correction = solved.reshape(PANELS * CB, columns_count)[coarse_index].reshape(sub_count, COR, columns_count)
        corrected = jnp.concatenate([residual[:, :COR, :] + correction, residual[:, COR:, :]], axis=1)
        norm_next = jnp.sum(residual * residual, axis=(0, 1))
        direction = corrected + (norm_next / norm_now) * direction
        norm_now = norm_next
    return residual, direction
```

```python
import jax
import jax.numpy as jnp
from jax import lax
from jax.experimental import pallas as pl
from jax.experimental.pallas import tpu as pltpu
from jax.sharding import Mesh
from jax.sharding import PartitionSpec as P

PANELS = 8
NY, NZ, NX, NC = 4, 8, 4, 2
BLOCKS = PANELS * (PANELS + 1) // 2
GRAN = 3
NGRAN = BLOCKS // GRAN
COLS = 8
BLK_GRP = ("blk_0", "blk_1", "blk_2", "grp")
BLK = ("blk_0", "blk_1", "blk_2")
MESH = pl.DeviceIdType.MESH
precise = lax.Precision.HIGHEST
f32 = jnp.float32
bf16 = jnp.bfloat16


def f_at(t, u):
    return t * (t + 1) // 2 + u


def d_at(t):
    return t * (t + 1) // 2 + t


BLOCK_OF = [(t, u) for t in range(PANELS) for u in range(t + 1)]


def kernel(
    order, f_ref, d_ref, pk, stat, r_ref, a_ref,
    sol_out, stat_out,
    fp, G, cin, cown, S, sbuf, rbuf, wbuf, opk, sol, stat_s, stat_r,
    st_send, st_recv, rl_send, rl_recv, dd_send, dd_recv,
    rd_send, rd_recv, c_send, c_recv, o_send, o_recv, t_send, t_recv,
):
    y = lax.axis_index("blk_0")
    z = lax.axis_index("blk_1")
    x = lax.axis_index("blk_2")
    c = lax.axis_index("grp")
    q = z * 2 + c
    znext = lax.rem(z + 1 - 2 * c + NZ, NZ)

    def dev(y=y, z=z, x=x, c=c):
        return {"blk_0": y, "blk_1": z, "blk_2": x, "grp": c}

    ypeers = [lax.rem(y + d, NY) for d in range(1, NY)]
    xpeers = [lax.rem(x + d, NX) for d in range(1, NX)]
    zcpeers = [
        (lax.rem(z + dz, NZ), lax.rem(c + dc, NC))
        for dz in range(NZ) for dc in range(NC) if dz or dc
    ]

    barrier = pltpu.get_barrier_semaphore()
    for p in ypeers:
        pl.semaphore_signal(barrier, inc=1, device_id=dev(y=p), device_id_type=MESH)
    for p in xpeers:
        pl.semaphore_signal(barrier, inc=1, device_id=dev(x=p), device_id_type=MESH)
    for pz, pc in zcpeers:
        pl.semaphore_signal(barrier, inc=1, device_id=dev(z=pz, c=pc), device_id_type=MESH)

    group = lax.broadcasted_iota(jnp.int32, (8, 128), 1) // 8 % 4
    for b, (t, u) in enumerate(BLOCK_OF):
        if u < t:
            row = f_ref[order[t] * PANELS + order[u]]
            for s in range(NY):
                fp[b, s] = row[:, 256 * s : 256 * s + 256]
        else:
            row = d_ref[order[t]]
            for s in range(NX):
                for zh in range(2):
                    piece = jnp.zeros((8, 128), f32)
                    for yy in range(NY):
                        nat = row[:, yy * 256 + zh * 128 : yy * 256 + zh * 128 + 128]
                        shift = (8 * (yy - s)) % 128
                        if shift:
                            nat = pltpu.roll(nat, shift, 1)
                        piece = jnp.where(group == yy, nat, piece)
                    fp[b, s, :, zh * 128 : zh * 128 + 128] = piece

    pl.semaphore_wait(barrier, len(ypeers) + len(xpeers) + len(zcpeers))

    def rcopy(src, dst, ss, rs, to):
        return pltpu.make_async_remote_copy(
            src_ref=src, dst_ref=dst, send_sem=ss, recv_sem=rs, device_id=to, device_id_type=MESH
        )

    me = dev(x=xpeers[0])

    def wait_recv(ref, sem):
        rcopy(ref, ref, sem, sem, me).wait_recv()

    def wait_send(ref, sem):
        rcopy(ref, ref, sem, sem, me).wait_send()

    for pz, pc in zcpeers:
        rcopy(pk.at[pz * 2 + pc], cin.at[q], c_send.at[0], c_recv.at[0], dev(z=pz, c=pc)).start()
    cin[q] = pk[q]

    def stage(g):
        for b in range(g * GRAN, g * GRAN + GRAN):
            t, u = BLOCK_OF[b]
            if u < t:
                G[b, z, y] = fp[b, y]
                for p in ypeers:
                    rcopy(fp.at[b, p], G.at[b, z, y], st_send.at[g], st_recv.at[g], dev(y=p)).start()
            else:
                G[b, z, x] = fp[b, x]
                for p in xpeers:
                    rcopy(fp.at[b, p], G.at[b, z, x], st_send.at[g], st_recv.at[g], dev(x=p)).start()

    def piece(g, h):
        zo = lax.rem(z - h * (1 - 2 * c) + NZ, NZ)
        if h == 4:
            return G.at[pl.ds(g * GRAN, GRAN), zo, pl.ds(2 * c, 2)]
        return G.at[pl.ds(g * GRAN, GRAN), zo]

    def send(g, h):
        ref = piece(g, h - 1)
        if h == 4:
            zo = lax.rem(z - 3 * (1 - 2 * c) + NZ, NZ)
            ref = G.at[pl.ds(g * GRAN, GRAN), zo, pl.ds(2 * c, 2)]
        rcopy(ref, ref, rl_send.at[g, h - 1], rl_recv.at[g, h - 1], dev(z=znext)).start()

    def share(g, h):
        ref = piece(g, h)
        rcopy(ref, ref, dd_send.at[g, h - 1], dd_recv.at[g, h - 1], dev(c=1 - c)).start()

    done = {"stage": 0, "slot": 0, "gran": 0}

    def stage_upto(n):
        while done["stage"] < min(n, NGRAN):
            stage(done["stage"])
            done["stage"] += 1

    def slots_upto(n):
        while done["slot"] < min(n, NGRAN + 4):
            k = done["slot"]
            stage_upto(k + 3)
            for h in range(4, -1, -1):
                g = k - h
                if not 0 <= g < NGRAN:
                    continue
                if h == 0:
                    wait_recv(fp.at[pl.ds(0, 3 * GRAN), 0], st_recv.at[g])
                    send(g, 1)
                else:
                    wait_recv(piece(g, h), rl_recv.at[g, h - 1])
                    if h < 4:
                        send(g, h + 1)
                    share(g, h)
            done["slot"] += 1

    def granules_upto(b):
        while done["gran"] * GRAN <= b:
            g = done["gran"]
            slots_upto(g + 5)
            for h in range(1, 5):
                zo = lax.rem(z + h * (1 - 2 * c) + NZ, NZ)
                ref = G.at[pl.ds(g * GRAN, GRAN), zo]
                if h == 4:
                    ref = G.at[pl.ds(g * GRAN, GRAN), zo, pl.ds(2 - 2 * c, 2)]
                wait_recv(ref, dd_recv.at[g, h - 1])
            done["gran"] += 1

    def product(v, b):
        block = G[b].reshape(256, 256)
        high = block.astype(bf16)
        low = (block - high.astype(f32)).astype(bf16)
        v_high = v.astype(bf16)
        v_low = (v - v_high.astype(f32)).astype(bf16)
        both = jnp.concatenate([v_high, v_low], axis=0)
        dims = (((1,), (1,)), ((), ()))
        first = lax.dot_general(both, high, dims, preferred_element_type=f32)
        second = lax.dot_general(v_high, low, dims, preferred_element_type=f32)
        return first[:16] + first[16:] + second

    def peers_of(phase):
        return [
            [dev(c=1 - c)],
            [dev(x=p) for p in xpeers],
            [dev(y=p) for p in ypeers],
            [dev(z=lax.rem(z + d, NZ)) for d in range(1, NZ)],
        ][phase % 4]

    def stat_send(phase):
        for d, to in enumerate(peers_of(phase)):
            rcopy(stat_s.at[phase], stat_r.at[phase, d], t_send.at[phase], t_recv.at[phase], to).start()

    def stat_take(phase):
        n = len(peers_of(phase))
        wait_recv(stat_r.at[phase, pl.ds(0, n)], t_recv.at[phase])
        total = stat_s[phase]
        for d in range(n):
            total = total + stat_r[phase, d]
        return total

    def stat_tick(tick):
        if tick == 0:
            stat_s[0] = stat[...]
            stat_send(0)
        elif tick < 8:
            total = stat_take(tick - 1)
            if tick == 4:
                stat_out[0] = total
                step = total[0:1] / total[1:2]

                def body(i, acc):
                    at = pl.ds(pl.multiple_of(i * 128, 128), 128)
                    new = r_ref[at, :] - step * a_ref[at, :]
                    return acc + jnp.sum((new * new).reshape(16, 8, 128), axis=0)

                acc = lax.fori_loop(0, 16, body, jnp.zeros((8, 128), f32))
                total = jnp.broadcast_to(jnp.sum(acc, axis=0, keepdims=True), (8, 128))
            stat_s[tick] = total
            stat_send(tick)
        elif tick == 8:
            stat_out[1] = stat_take(7)

    def exchange(tick, value, targets):
        sbuf[tick] = value
        for d, to in enumerate(targets):
            rcopy(sbuf.at[tick], rbuf.at[tick, d], rd_send.at[tick], rd_recv.at[tick], to).start()

    def finish(tick):
        wait_recv(rbuf.at[tick], rd_recv.at[tick])
        return (sbuf[tick] + rbuf[tick, 0]) + (rbuf[tick, 1] + rbuf[tick, 2])

    stage_upto(3)
    slots_upto(2)

    wait_recv(cin.at[pl.ds(0, NZ * NC - 1)], c_recv.at[0])
    lane = lax.broadcasted_iota(jnp.int32, (8, 128), 1)
    quads = [cin[2 * zz] + cin[2 * zz + 1] for zz in range(NZ)]

    def own(k, t):
        halves = []
        for zh in range(2):
            acc = jnp.zeros((8, 128), f32)
            for zl in range(4):
                src = quads[zh * 4 + zl]
                shift = (zl * 32 - (k * 64 + t * 8)) % 128
                if shift:
                    src = pltpu.roll(src, shift, 1)
                acc = jnp.where((lane >= zl * 32) & (lane < zl * 32 + 8), src, acc)
            halves.append(pltpu.roll(acc, y * 8, 1))
        return halves

    for t in range(PANELS):
        for k in range(2):
            for zh, half in enumerate(own(k, t)):
                cown[t, k * 8 : k * 8 + 8, zh * 128 : zh * 128 + 128] = half

    pending = cown[0]
    for t in range(PANELS):
        tick = 2 * t
        if t:
            pending = pending - product(S[t - 1], f_at(t, t - 1))
        exchange(tick, pending, [dev(y=p) for p in ypeers])
        stat_tick(tick)
        slots_upto(tick + 3)
        granules_upto(d_at(t))
        target = finish(tick)

        tick += 1
        exchange(tick, product(target, d_at(t)), [dev(x=p) for p in xpeers])
        stat_tick(tick)
        slots_upto(tick + 3)
        if t + 1 < PANELS:
            granules_upto(f_at(t + 1, t))
            pending = cown[t + 1]
            for u in range(t):
                pending = pending - product(S[u], f_at(t + 1, u))
        S[t] = finish(tick)
        back = lax.rem(128 - 8 * x, 128)
        for k in range(2):
            for zh in range(2):
                wbuf[t, k, zh] = pltpu.roll(S[t, k * 8 : k * 8 + 8, zh * 128 : zh * 128 + 128], back, 1)

    for zz in range(NZ):
        acc = jnp.zeros((8, 128), f32)
        for t in range(PANELS):
            for k in range(2):
                src = wbuf[t, k, zz // 4]
                shift = (k * 64 + t * 8 - (zz % 4) * 32) % 128
                if shift:
                    src = pltpu.roll(src, shift, 1)
                at = k * 64 + t * 8
                acc = jnp.where((lane >= at) & (lane < at + 8), src, acc)
        opk[zz] = acc
    for pz, pc in zcpeers:
        rcopy(opk.at[pz], sol.at[q], o_send.at[0], o_recv.at[0], dev(z=pz, c=pc)).start()
    sol[q] = opk[z]
    wait_recv(sol.at[pl.ds(0, NZ * NC - 1)], o_recv.at[0])
    sol_out[...] = sol[...]

    wait_send(cin.at[pl.ds(0, NZ * NC - 1)], c_send.at[0])
    wait_send(sol.at[pl.ds(0, NZ * NC - 1)], o_send.at[0])
    for g in range(NGRAN):
        wait_send(fp.at[pl.ds(0, 3 * GRAN), 0], st_send.at[g])
        for h in range(1, 5):
            wait_send(piece(g, h), rl_send.at[g, h - 1])
            wait_send(piece(g, h), dd_send.at[g, h - 1])
    for tick in range(2 * PANELS):
        wait_send(rbuf.at[tick], rd_send.at[tick])
    for phase in range(8):
        wait_send(stat_r.at[phase, pl.ds(0, len(peers_of(phase)))], t_send.at[phase])


def coarse_kernel(order, f_own, d_own, pk, stat, r, a):
    vmem = pl.BlockSpec(memory_space=pltpu.VMEM)
    smem = pl.BlockSpec(memory_space=pltpu.SMEM)
    dma = pltpu.SemaphoreType.DMA
    return pl.pallas_call(
        kernel,
        out_shape=(
            jax.ShapeDtypeStruct((16, 8, 128), f32),
            jax.ShapeDtypeStruct((2, 8, 128), f32),
        ),
        in_specs=[smem] + [vmem] * 6,
        out_specs=(vmem, vmem),
        scratch_shapes=[
            pltpu.VMEM((BLOCKS, 4, 8, 256), f32),
            pltpu.VMEM((BLOCKS, NZ, 4, 8, 256), f32),
            pltpu.VMEM((16, 8, 128), f32),
            pltpu.VMEM((PANELS, 16, 256), f32),
            pltpu.VMEM((PANELS, 16, 256), f32),
            pltpu.VMEM((2 * PANELS, 16, 256), f32),
            pltpu.VMEM((2 * PANELS, 3, 16, 256), f32),
            pltpu.VMEM((PANELS, 2, 2, 8, 128), f32),
            pltpu.VMEM((NZ, 8, 128), f32),
            pltpu.VMEM((16, 8, 128), f32),
            pltpu.VMEM((8, 8, 128), f32),
            pltpu.VMEM((8, 7, 8, 128), f32),
            dma((NGRAN,)), dma((NGRAN,)),
            dma((NGRAN, 4)), dma((NGRAN, 4)),
            dma((NGRAN, 4)), dma((NGRAN, 4)),
            dma((2 * PANELS,)), dma((2 * PANELS,)),
            dma((1,)), dma((1,)),
            dma((1,)), dma((1,)),
            dma((8,)), dma((8,)),
        ],
        compiler_params=pltpu.CompilerParams(
            collective_id=0, has_side_effects=True, vmem_limit_bytes=40 * 1024 * 1024
        ),
    )(order, f_own, d_own, pk, stat, r, a)


def local(
    schur_blocks, residual, direction, corner_map, panel_order, coarse_factor, block_inverses
):
    sub_count, rows, columns = residual.shape
    corners = corner_map.shape[1]
    position = jnp.zeros((PANELS,), jnp.int32).at[panel_order].set(jnp.arange(PANELS, dtype=jnp.int32))
    hot = (corner_map[:, :, None] // 8 == jnp.arange(PANELS, dtype=jnp.int32)).astype(jnp.int32)
    slot = jnp.sum(hot * position, axis=-1) * 8 + corner_map % 8
    placing = (slot[:, :, None] == lax.broadcasted_iota(jnp.int32, (1, 1, 64), 2)).astype(f32)
    applied = jnp.einsum(
        "sij,sjv->siv", schur_blocks, direction.astype(bf16), preferred_element_type=f32
    )
    rr = jnp.sum(residual * residual, axis=(0, 1))
    curvature = jnp.sum(direction * applied, axis=(0, 1))
    stat = jnp.concatenate([rr[None], curvature[None], jnp.zeros((6, columns), f32)], axis=0)
    pk_r = jnp.einsum("scm,scv->vm", placing, residual[:, :corners], precision=precise)
    pk_a = jnp.einsum("scm,scv->vm", placing, applied[:, :corners], precision=precise)
    pk = jnp.concatenate([pk_r, pk_a], axis=1).reshape(16, 8, 128)
    sol, stats = coarse_kernel(
        panel_order,
        coarse_factor.reshape(PANELS * PANELS, 8, 1024),
        block_inverses,
        pk,
        stat,
        residual.reshape(-1, columns),
        applied.reshape(-1, columns),
    )
    norm_now = stats[0, 0]
    step = norm_now / stats[0, 1]
    norm_next = stats[1, 0]
    flat = sol.reshape(columns, 128)
    solved = flat[:, :64] - step[:, None] * flat[:, 64:]
    residual = residual - step * applied
    correction = jnp.einsum("scm,vm->scv", placing, solved, precision=precise)
    corrected = jnp.concatenate(
        [residual[:, :corners] + correction, residual[:, corners:]], axis=1
    )
    direction = corrected + norm_next / norm_now * direction
    return residual, direction


def solution(mesh):
    split = Mesh(
        mesh.devices.reshape(NY, NZ, NX, NC), ("blk_0", "blk_1", "blk_2", "grp")
    )
    placed = (
        P(BLK_GRP, None, None),
        P(BLK_GRP, None, None),
        P(BLK_GRP, None, None),
        P(BLK_GRP, None),
        P(),
        P(None, None, BLK, None),
        P(None, BLK, None),
    )
    return jax.shard_map(
        local,
        mesh=split,
        in_specs=placed,
        out_specs=(P(BLK_GRP, None, None), P(BLK_GRP, None, None)),
        check_vma=False,
    )
```
